32 devices in a mesh: e: 4 (over z), b: 2 (over y), a: 4 (over x, core).
Axes of the slice: x: 2, y: 2, z: 4, core: 2. Of those that a mesh axis runs over, the one named last changes fastest.
Arguments:
- act_in: bfloat16 [32, 256, 1536], P(('a', 'b'), None, 'e')
- grad_y: bfloat16 [32, 256, 1536], P(('a', 'b'), None, 'e')
- ln1_gain: float32 [1536], P('e')
- ln1_shift: float32 [1536], P('e')
- w_qkv: bfloat16 [3, 1536, 1536], P(None, 'e', ('b', 'a'))
- b_qkv: float32 [3, 16, 96], P(None, 'b')
- w_out: bfloat16 [1536, 1536], P('b', ('e', 'a'))
- b_out: float32 [1536], P('e')
- ln2_gain: float32 [1536], P('e')
- ln2_shift: float32 [1536], P('e')
- w_up: bfloat16 [1536, 6144], P('e', ('b', 'a'))
- b_up: float32 [6144], P('b')
- w_down: bfloat16 [6144, 1536], P('b', ('e', 'a'))
- b_down: float32 [1536], P('e')
Outputs:
- output 1: bfloat16 [32, 256, 1536], P(('a', 'b'), None, 'e')
- output 2: bfloat16 [32, 256, 1536], P(('a', 'b'), None, 'e')
- output 3: float32 [1536], P('e')
- output 4: float32 [1536], P('e')
- output 5: bfloat16 [3, 1536, 1536], P(None, 'e', ('b', 'a'))
- output 6: float32 [3, 16, 96], P(None, 'b')
- output 7: bfloat16 [1536, 1536], P('b', ('e', 'a'))
- output 8: float32 [1536], P('e')
- output 9: float32 [1536], P('e')
- output 10: float32 [1536], P('e')
- output 11: bfloat16 [1536, 6144], P('e', ('b', 'a'))
- output 12: float32 [6144], P('b')
- output 13: bfloat16 [6144, 1536], P('b', ('e', 'a'))
- output 14: float32 [1536], P('e')
All inputs are finite; a program needn't handle non-finite values.
Results may differ from the reference program's by a relative error of at most 0.02.
Values are sent between devices in bfloat16 or wider.
A program may use at most 1 GiB of HBM per device.

```python
import jax
import jax.numpy as jnp
from jax import lax

BATCH_SEQS = 32
SEQ_LEN = 256
HIDDEN = 1536
N_HEADS = 16
HEAD_DIM = 96
FFN_DIM = 6144
LN_EPS = 1e-5


def setup_inputs(seed: int = 0) -> dict:
    sub_keys = jax.random.split(jax.random.key(seed), 16)
    act_shape = (BATCH_SEQS, SEQ_LEN, HIDDEN)
    col_ramp = jnp.linspace(-1.0, 1.0, HIDDEN, dtype=jnp.float32)
    row_amp = jax.random.normal(sub_keys[0], (BATCH_SEQS, SEQ_LEN, 1), jnp.float32)
    x_noise = jax.random.normal(sub_keys[1], act_shape, jnp.float32)
    hid_scale = HIDDEN ** -0.5
    ffn_scale = FFN_DIM ** -0.5
    return {
        'act_in': (x_noise + row_amp * col_ramp).astype(jnp.bfloat16),
        'grad_y': jax.random.normal(sub_keys[2], act_shape, jnp.float32).astype(jnp.bfloat16),
        'ln1_gain': 1.0 + 0.3 * jax.random.normal(sub_keys[3], (HIDDEN,), jnp.float32),
        'ln1_shift': 0.3 * jax.random.normal(sub_keys[4], (HIDDEN,), jnp.float32),
        'w_qkv': (jax.random.normal(sub_keys[5], (3, HIDDEN, HIDDEN), jnp.float32) * hid_scale).astype(jnp.bfloat16),
        'b_qkv': 0.5 * jax.random.normal(sub_keys[6], (3, N_HEADS, HEAD_DIM), jnp.float32),
        'w_out': (jax.random.normal(sub_keys[7], (HIDDEN, HIDDEN), jnp.float32) * hid_scale).astype(jnp.bfloat16),
        'b_out': 0.5 * jax.random.normal(sub_keys[8], (HIDDEN,), jnp.float32),
        'ln2_gain': 1.0 + 0.3 * jax.random.normal(sub_keys[9], (HIDDEN,), jnp.float32),
        'ln2_shift': 0.3 * jax.random.normal(sub_keys[10], (HIDDEN,), jnp.float32),
        'w_up': (jax.random.normal(sub_keys[11], (HIDDEN, FFN_DIM), jnp.float32) * hid_scale).astype(jnp.bfloat16),
        'b_up': 0.5 * jax.random.normal(sub_keys[12], (FFN_DIM,), jnp.float32),
        'w_down': (jax.random.normal(sub_keys[13], (FFN_DIM, HIDDEN), jnp.float32) * ffn_scale).astype(jnp.bfloat16),
        'b_down': 0.5 * jax.random.normal(sub_keys[14], (HIDDEN,), jnp.float32),
    }


def f32_dot(left_op, right_op):
    return jnp.dot(left_op.astype(jnp.float32), right_op.astype(jnp.float32))


def layer_norm(x_wide, ln_gain, ln_shift):
    row_mean = jnp.mean(x_wide, axis=-1, keepdims=True)
    centered = x_wide - row_mean
    variance = jnp.mean(centered * centered, axis=-1, keepdims=True)
    return centered * lax.rsqrt(variance + LN_EPS) * ln_gain + ln_shift


def attend_sequence(qkv_trio):
    q_seq, k_seq, v_seq = qkv_trio
    scores = jnp.einsum('qhd,khd->hqk', q_seq.astype(jnp.float32), k_seq.astype(jnp.float32)) * (HEAD_DIM ** -0.5)
    causal = jnp.arange(SEQ_LEN)[:, None] >= jnp.arange(SEQ_LEN)[None, :]
    scores = jnp.where(causal, scores, -1e30)
    attn_probs = jax.nn.softmax(scores, axis=-1).astype(jnp.bfloat16)
    context = jnp.einsum('hqk,khd->qhd', attn_probs.astype(jnp.float32), v_seq.astype(jnp.float32))
    return context.astype(jnp.bfloat16)


def layer_forward(act_in, ln1_gain, ln1_shift, w_qkv, b_qkv, w_out, b_out, ln2_gain, ln2_shift, w_up, b_up, w_down, b_down):
    n_tokens = BATCH_SEQS * SEQ_LEN
    heads_shape = (BATCH_SEQS, SEQ_LEN, N_HEADS, HEAD_DIM)
    x_rows = act_in.reshape(n_tokens, HIDDEN).astype(jnp.float32)
    h_one = layer_norm(x_rows, ln1_gain, ln1_shift).astype(jnp.bfloat16)
    q_all = (f32_dot(h_one, w_qkv[0]) + b_qkv[0].reshape(HIDDEN)).astype(jnp.bfloat16).reshape(heads_shape)
    k_all = (f32_dot(h_one, w_qkv[1]) + b_qkv[1].reshape(HIDDEN)).astype(jnp.bfloat16).reshape(heads_shape)
    v_all = (f32_dot(h_one, w_qkv[2]) + b_qkv[2].reshape(HIDDEN)).astype(jnp.bfloat16).reshape(heads_shape)
    context = lax.map(jax.checkpoint(attend_sequence), (q_all, k_all, v_all)).reshape(n_tokens, HIDDEN)
    x_one = (x_rows + f32_dot(context, w_out) + b_out).astype(jnp.bfloat16)
    h_two = layer_norm(x_one.astype(jnp.float32), ln2_gain, ln2_shift).astype(jnp.bfloat16)
    mlp_act = jax.nn.gelu(f32_dot(h_two, w_up) + b_up, approximate=True).astype(jnp.bfloat16)
    y_rows = (x_one.astype(jnp.float32) + f32_dot(mlp_act, w_down) + b_down).astype(jnp.bfloat16)
    return y_rows.reshape(BATCH_SEQS, SEQ_LEN, HIDDEN)


def reference(act_in, grad_y, ln1_gain, ln1_shift, w_qkv, b_qkv, w_out, b_out, ln2_gain, ln2_shift, w_up, b_up, w_down, b_down):
    y_out, pullback = jax.vjp(layer_forward, act_in, ln1_gain, ln1_shift, w_qkv, b_qkv, w_out, b_out, ln2_gain, ln2_shift, w_up, b_up, w_down, b_down)
    (grad_x, grad_ln1_gain, grad_ln1_shift, grad_w_qkv, grad_b_qkv, grad_w_out, grad_b_out,
     grad_ln2_gain, grad_ln2_shift, grad_w_up, grad_b_up, grad_w_down, grad_b_down) = pullback(grad_y)
    return (y_out, grad_x, grad_ln1_gain, grad_ln1_shift, grad_w_qkv, grad_b_qkv, grad_w_out, grad_b_out,
            grad_ln2_gain, grad_ln2_shift, grad_w_up, grad_b_up, grad_w_down, grad_b_down)
```

```python
import jax
import jax.numpy as jnp
from jax import lax
from jax.experimental import pallas as pl
from jax.experimental.pallas import tpu as pltpu
from jax.sharding import PartitionSpec as P

LN_EPS = 1e-5
F32 = jnp.float32
BF16 = jnp.bfloat16


def norm_forward(x_wide, gain, shift):
    hidden = x_wide.shape[-1]
    row_mean = jnp.sum(x_wide, axis=-1, keepdims=True) / hidden
    centered = x_wide - row_mean
    variance = jnp.sum(centered * centered, axis=-1, keepdims=True) / hidden
    inv_std = lax.rsqrt(variance + LN_EPS)
    normed = centered * inv_std
    return (normed * gain + shift).astype(BF16), normed, inv_std


def norm_backward(d_out, normed, inv_std, gain):
    hidden = d_out.shape[-1]
    d_normed = d_out * gain
    s0 = jnp.sum(d_normed, axis=-1, keepdims=True) / hidden
    s1 = jnp.sum(d_normed * normed, axis=-1, keepdims=True) / hidden
    d_in = inv_std * (d_normed - s0 - normed * s1)
    return d_in, jnp.sum(d_out * normed, axis=0), jnp.sum(d_out, axis=0)


def lane_ids(shape):
    return lax.broadcasted_iota(jnp.int32, shape, 1)


def head_probs(q_head, k, causal, scale):
    scores = lax.dot_general(q_head, k, (((1,), (1,)), ((), ())), preferred_element_type=F32) * scale
    scores = jnp.where(causal, scores, -1e30)
    probs = jnp.exp(scores - jnp.max(scores, axis=1, keepdims=True))
    return probs * (1.0 / jnp.sum(probs, axis=1, keepdims=True))


def attention_kernel(n_heads, head_dim, qkv_ref, ctx_ref):
    seq_len, slot = ctx_ref.shape
    q, k, v = [qkv_ref[:, g * slot:(g + 1) * slot] for g in range(3)]
    causal = lax.broadcasted_iota(jnp.int32, (seq_len, seq_len), 0) >= lane_ids((seq_len, seq_len))
    lanes = lane_ids((seq_len, slot))
    context = jnp.zeros((seq_len, slot), F32)
    for h in range(n_heads):
        mine = (lanes >= h * head_dim) & (lanes < (h + 1) * head_dim)
        probs = head_probs(jnp.where(mine, q, jnp.zeros_like(q)), k, causal, head_dim ** -0.5).astype(BF16)
        context = jnp.where(mine, jnp.dot(probs, v, preferred_element_type=F32), context)
    ctx_ref[...] = context.astype(BF16)


def attention_grad_kernel(n_heads, head_dim, qkv_ref, dctx_ref, dqkv_ref):
    seq_len, slot = dctx_ref.shape
    q, k, v = [qkv_ref[:, g * slot:(g + 1) * slot] for g in range(3)]
    d_ctx = dctx_ref[...]
    causal = lax.broadcasted_iota(jnp.int32, (seq_len, seq_len), 0) >= lane_ids((seq_len, seq_len))
    lanes = lane_ids((seq_len, slot))
    scale = head_dim ** -0.5
    d_q, d_k, d_v = [jnp.zeros((seq_len, slot), F32) for _ in range(3)]
    for h in range(n_heads):
        mine = (lanes >= h * head_dim) & (lanes < (h + 1) * head_dim)
        q_head = jnp.where(mine, q, jnp.zeros_like(q))
        d_head = jnp.where(mine, d_ctx, jnp.zeros_like(d_ctx))
        probs = head_probs(q_head, k, causal, scale)
        d_v += lax.dot_general(probs.astype(BF16), d_head, (((0,), (0,)), ((), ())), preferred_element_type=F32)
        d_probs = lax.dot_general(d_head, v, (((1,), (1,)), ((), ())), preferred_element_type=F32)
        d_probs = d_probs.astype(BF16).astype(F32)
        d_scores = probs * (d_probs - jnp.sum(d_probs * probs, axis=1, keepdims=True)) * scale
        d_scores = d_scores.astype(BF16)
        d_q = jnp.where(mine, jnp.dot(d_scores, k, preferred_element_type=F32), d_q)
        d_k += lax.dot_general(d_scores, q_head, (((0,), (0,)), ((), ())), preferred_element_type=F32)
    for g, d in enumerate((d_q, d_k, d_v)):
        dqkv_ref[:, g * slot:(g + 1) * slot] = d.astype(BF16)


def attention(qkv, n_b, seq_len, n_heads, head_dim):
    t, width = qkv.shape[0], qkv.shape[1] // n_b
    slot = width // 3
    n = n_b * t // seq_len
    return pl.pallas_call(
        lambda *refs: attention_kernel(n_heads, head_dim, *refs),
        grid=(t // seq_len, n_b),
        out_shape=jax.ShapeDtypeStruct((t, n_b * slot), BF16),
        in_specs=[pl.BlockSpec((seq_len, width), lambda i, j: (i, j))],
        out_specs=pl.BlockSpec((seq_len, slot), lambda i, j: (i, j)),
        cost_estimate=pl.CostEstimate(flops=4 * n * n_heads * seq_len * seq_len * slot, bytes_accessed=n * seq_len * (width + slot) * 2, transcendentals=n * n_heads * seq_len * seq_len),
        name="attention",
    )(qkv)


def attention_grad(qkv, d_ctx, n_b, seq_len, n_heads, head_dim):
    t, width = qkv.shape[0], qkv.shape[1] // n_b
    slot = width // 3
    n = n_b * t // seq_len
    return pl.pallas_call(
        lambda *refs: attention_grad_kernel(n_heads, head_dim, *refs),
        grid=(t // seq_len, n_b),
        out_shape=jax.ShapeDtypeStruct(qkv.shape, BF16),
        in_specs=[pl.BlockSpec((seq_len, width), lambda i, j: (i, j)),
                  pl.BlockSpec((seq_len, slot), lambda i, j: (i, j))],
        out_specs=pl.BlockSpec((seq_len, width), lambda i, j: (i, j)),
        cost_estimate=pl.CostEstimate(flops=10 * n * n_heads * seq_len * seq_len * slot, bytes_accessed=n * seq_len * (2 * width + slot) * 2, transcendentals=n * n_heads * seq_len * seq_len),
        name="attention_grad",
    )(qkv, d_ctx)


def cat(refs):
    return jnp.concatenate([r[...] for r in refs], axis=0)


def tn(left, right):
    return lax.dot_general(left, right, (((0,), (0,)), ((), ())), preferred_element_type=F32)


def weight_grad(lefts, right, b, block):
    m, k = lefts[0].shape
    t = m * len(lefts)
    n = right.shape[1] // b

    def kernel(*refs):
        refs[-1][0] = tn(cat(refs[:-2]), refs[-2][...]).astype(BF16)

    return pl.pallas_call(
        kernel,
        grid=(b, k // block),
        out_shape=jax.ShapeDtypeStruct((b, k, n), BF16),
        in_specs=[pl.BlockSpec((m, block), lambda i, j: (0, j))] * len(lefts) + [pl.BlockSpec((t, n), lambda i, j: (0, i))],
        out_specs=pl.BlockSpec((1, block, n), lambda i, j: (i, j, 0)),
        cost_estimate=pl.CostEstimate(flops=2 * b * t * k * n, bytes_accessed=2 * (b * t * k + b * t * n + b * k * n), transcendentals=0),
        name="weight_grad",
    )(*lefts, right)


def attn_weight_grad(hs, d_qkv, d_xs, ctx, b, block):
    m, k = hs[0].shape
    parts = len(hs)
    t = m * parts
    n = d_qkv.shape[1] // b
    slot = n // 3
    used = slot * 3 // 4

    def kernel(*refs):
        h, d_x = cat(refs[:parts]), cat(refs[parts:2 * parts])
        dqkv_ref, ctx_ref, out_ref = refs[2 * parts:]
        d_out = tn(d_x, ctx_ref[...])
        lanes = lane_ids(d_out.shape)
        for g in range(3):
            moved = pltpu.roll(d_out, (used - g * (slot - used)) % slot, 1)
            d = tn(h, dqkv_ref[:, g * slot:(g + 1) * slot])
            out_ref[0, :, g * slot:(g + 1) * slot] = jnp.where(lanes >= used, moved, d).astype(BF16)

    return pl.pallas_call(
        kernel,
        grid=(b, k // block),
        out_shape=jax.ShapeDtypeStruct((b, k, n), BF16),
        in_specs=[pl.BlockSpec((m, block), lambda i, j: (0, j))] * (2 * parts)
        + [pl.BlockSpec((t, n), lambda i, j: (0, i)), pl.BlockSpec((t, slot), lambda i, j: (0, i))],
        out_specs=pl.BlockSpec((1, block, n), lambda i, j: (i, j, 0)),
        cost_estimate=pl.CostEstimate(flops=2 * b * t * k * (n + slot), bytes_accessed=2 * (2 * b * t * k + b * t * n + b * k * n), transcendentals=0),
        name="attn_weight_grad",
    )(*hs, *d_xs, d_qkv, ctx)


GELU_C = 0.7978845608028654


def times(lefts, w, tile, epilogue, extras=()):
    m, k = lefts[0].shape
    parts = len(lefts)
    t = m * parts
    b, _, n = w.shape
    steps = n // tile
    wide = lambda i, j: (0, i * steps + j)
    outs = {'plain': [(t, BF16)], 'bias': [(t, BF16)], 'gelu': [(t, F32), (t, BF16)], 'gelu_grad': [(t, BF16), (1, F32)]}[epilogue]

    def kernel(*refs):
        w_ref = refs[parts]
        extra = refs[parts + 1:parts + 1 + len(extras)]
        out = refs[parts + 1 + len(extras):-1]
        rows = refs[-1]

        @pl.when((pl.program_id(0) == 0) & (pl.program_id(1) == 0))
        def _():
            for r in range(parts):
                rows[r * m:(r + 1) * m, :] = refs[r][...]

        y = jnp.dot(rows[...], w_ref[0], preferred_element_type=F32)
        if epilogue == 'plain':
            out[0][...] = y.astype(BF16)
        elif epilogue == 'bias':
            out[0][...] = (y + extra[0][...]).astype(BF16)
        elif epilogue == 'gelu':
            y = y + extra[0][...]
            out[0][...] = y
            out[1][...] = (y * (0.5 * (1.0 + jnp.tanh(GELU_C * (y + 0.044715 * (y * y * y)))))).astype(BF16)
        else:
            d = y.astype(BF16).astype(F32)
            x = extra[0][...]
            th = jnp.tanh(GELU_C * (x + 0.044715 * (x * x * x)))
            slope = 0.5 * (1.0 + th) + 0.5 * x * (1.0 - th * th) * (GELU_C * (1.0 + 3 * 0.044715 * (x * x)))
            d = d * slope
            out[0][...] = d.astype(BF16)
            out[1][...] = jnp.sum(d, axis=0, keepdims=True)

    res = pl.pallas_call(
        kernel,
        grid=(b, steps),
        out_shape=[jax.ShapeDtypeStruct((r, b * n), d) for r, d in outs],
        in_specs=[pl.BlockSpec((m, k), lambda i, j: (0, 0))] * parts + [pl.BlockSpec((1, k, tile), lambda i, j: (i, 0, j))]
        + [pl.BlockSpec((x.shape[0], tile), wide) for x in extras],
        out_specs=[pl.BlockSpec((r, tile), wide) for r, d in outs],
        scratch_shapes=[pltpu.VMEM((t, k), BF16)],
        cost_estimate=pl.CostEstimate(flops=2 * b * t * k * n, bytes_accessed=2 * (t * k + b * k * n + 2 * b * t * n), transcendentals=0),
        name="times_" + epilogue,
    )(*lefts, w, *extras)
    return res[0] if len(outs) == 1 else res


def times_t(left, w, tile, parts):
    t = left.shape[0]
    b, k, n = w.shape
    m = t // parts

    def kernel(left_ref, w_ref, *out):
        y = sum(lax.dot_general(left_ref[:, i * n:(i + 1) * n], w_ref[i], (((1,), (1,)), ((), ())), preferred_element_type=F32) for i in range(b))
        for r in range(parts):
            out[r][...] = y[r * m:(r + 1) * m].astype(BF16)

    return pl.pallas_call(
        kernel,
        grid=(k // tile,),
        out_shape=[jax.ShapeDtypeStruct((m, k), BF16)] * parts,
        in_specs=[pl.BlockSpec((t, b * n), lambda j: (0, 0)), pl.BlockSpec((b, tile, n), lambda j: (0, j, 0))],
        out_specs=[pl.BlockSpec((m, tile), lambda j: (0, j))] * parts,
        cost_estimate=pl.CostEstimate(flops=2 * b * t * k * n, bytes_accessed=2 * (t * k + b * k * n + b * t * n), transcendentals=0),
        name="times_t",
    )(left, w)


def solution(mesh):
    NE, NB, NA = mesh.shape['e'], mesh.shape['b'], mesh.shape['a']
    spec_act = P(('a', 'b'), None, 'e')
    spec_col_e = P('e')
    spec_col_b = P('b')
    spec_qkv = P(None, 'e', ('b', 'a'))
    spec_qkv_bias = P(None, 'b', None)
    spec_rows_b = P('b', ('e', 'a'))
    spec_rows_e = P('e', ('b', 'a'))
    all_specs = (spec_act, spec_act, spec_col_e, spec_col_e, spec_qkv, spec_qkv_bias, spec_rows_b,
                 spec_col_e, spec_col_e, spec_col_e, spec_rows_e, spec_col_b, spec_rows_b, spec_col_e)

    def from_e(t, k):
        return lax.ppermute(t, 'e', [((i + k) % NE, i) for i in range(NE)])

    def to_e(t, k):
        return lax.ppermute(t, 'e', [(i, (i + k) % NE) for i in range(NE)])

    def swap_b(t):
        return lax.ppermute(t, 'b', [(0, 1), (1, 0)])

    def swap_a(t, r):
        return lax.ppermute(t, 'a', [(i, i ^ r) for i in range(NA)])

    def pick(t, i):
        return lax.dynamic_index_in_dim(t, i, 0, keepdims=False)

    def local_step(x_loc, dy_loc, ln1_gain, ln1_shift, w_qkv, b_qkv, w_out, b_out, ln2_gain, ln2_shift, w_up, b_up, w_down, b_down):
        e_idx, b_idx, a_idx = lax.axis_index('e'), lax.axis_index('b'), lax.axis_index('a')
        n_seq, seq_len, cols_e = x_loc.shape
        heads_b, head_dim = b_qkv.shape[1], b_qkv.shape[2]
        heads_a = heads_b // NA

        def rows_in(t):
            got = [pick(t, e_idx)]
            got += [from_e(pick(t, (e_idx - k) % NE), k) for k in range(1, NE)]
            got = jnp.stack(got)
            return jnp.concatenate([pick(got, (j - e_idx) % NE) for j in range(NE)], axis=-1)

        def rows_out(t):
            blocks = jnp.stack([t[:, j * cols_e:(j + 1) * cols_e] for j in range(NE)])
            got = [pick(blocks, e_idx)] + [to_e(pick(blocks, (e_idx + k) % NE), k) for k in range(1, NE)]
            got = jnp.stack(got)
            return jnp.stack([pick(got, (e_idx - j) % NE) for j in range(NE)])

        def gather_eb(blk):
            full = lax.all_gather(blk, ('b', 'e'), axis=0, tiled=True)
            return full.reshape(NB, NE * blk.shape[0], blk.shape[1])

        def reduce_eb(part):
            return lax.psum_scatter(part.reshape(NB * part.shape[1], part.shape[2]), ('b', 'e'), scatter_dimension=0, tiled=True)

        def reduce_eb_steps(part):
            part = part.reshape(NB, NE, cols_e, part.shape[2])
            order = (1, 3, 2, 0)
            mine, theirs = pick(part, b_idx), pick(part, 1 - b_idx)
            total = {k: pick(mine, (e_idx + k) % NE).astype(F32) + swap_b(pick(theirs, (e_idx + k) % NE)).astype(F32) for k in order}
            out = total[0]
            for k in (1, 3, 2):
                out = out + to_e(total[k].astype(BF16), k).astype(F32)
            return out.astype(BF16)

        def gather_a(t):
            t2 = swap_a(t, 2)
            return [t, swap_a(t, 1), t2, swap_a(t2, 1)]

        def scatter_a(parts):
            p0, p1, p2, p3 = parts
            q2 = (p2.astype(F32) + swap_a(p3, 1).astype(F32)).astype(BF16)
            far = swap_a(q2, 2)
            return p0.astype(F32) + swap_a(p1, 1).astype(F32) + far.astype(F32)

        def rows_to_cols_a(w):
            blocks = w.reshape(NA, w.shape[0] // NA, w.shape[1])
            blocks = jnp.transpose(blocks, (0, 2, 1))
            rel = [pick(blocks, a_idx)] + [swap_a(pick(blocks, a_idx ^ r), r) for r in range(1, NA)]
            rel = jnp.stack(rel)
            return jnp.concatenate([pick(rel, j ^ a_idx) for j in range(NA)], axis=0)

        def cols_to_rows_a(w):
            blocks = w.reshape(NA, w.shape[0] // NA, w.shape[1])
            rel = [pick(blocks, a_idx)] + [swap_a(pick(blocks, a_idx ^ r), r) for r in range(1, NA)]
            rel = jnp.stack(rel)
            rel = jnp.stack([pick(rel, j ^ a_idx) for j in range(NA)])
            return jnp.transpose(rel, (0, 2, 1)).reshape(NA * w.shape[1], w.shape[0] // NA)

        nq = w_qkv.shape[2]
        nfill = nq // 3
        out_blk = rows_to_cols_a(w_out)
        qo_blk = jnp.concatenate([t for g in range(3) for t in (w_qkv[g], out_blk[:, g * nfill:(g + 1) * nfill])], axis=1)
        slot = nq + nfill
        wq = gather_eb(qo_blk)
        wo = jnp.concatenate([wq[:, :, g * slot + nq:(g + 1) * slot] for g in range(3)] + [jnp.zeros((NB, wq.shape[1], nfill), BF16)], axis=2)
        wu = gather_eb(w_up)
        wd = gather_eb(rows_to_cols_a(w_down))
        nu = wu.shape[2]

        x_row = rows_in(x_loc)
        vecs = jnp.stack([ln1_gain, ln1_shift, ln2_gain, ln2_shift, b_out, b_down])
        vecs = jnp.stack([vecs] + [from_e(vecs, k) for k in range(1, NE)])
        vecs = jnp.concatenate([pick(vecs, (j - e_idx) % NE) for j in range(NE)], axis=1)
        g1, s1, g2, s2, bo, bd = [vecs[i:i + 1] for i in range(6)]
        def both_b(v):
            other = swap_b(v)
            return jnp.stack([jnp.where(b_idx == 0, v, other), jnp.where(b_idx == 0, other, v)])

        bq = lax.dynamic_index_in_dim(b_qkv.reshape(3, NA, nq), a_idx, 1, keepdims=False)
        bq = jnp.pad(bq, ((0, 0), (0, nfill))).reshape(1, 3 * slot)
        bq = both_b(bq).reshape(1, NB * 3 * slot)
        bu = both_b(lax.dynamic_index_in_dim(b_up.reshape(NA, b_up.shape[0] // NA), a_idx, 0, keepdims=True)).reshape(1, NB * nu)

        tile = slot

        x_wide = x_row.astype(F32)
        h_one, normed_one, inv_one = norm_forward(x_wide, g1, s1)
        h_one_all = gather_a(h_one)
        dy_row = rows_in(dy_loc)
        dy_all = gather_a(dy_row)
        h_one_all, dy_all = lax.optimization_barrier((h_one_all, dy_all))
        qkv = times(h_one_all, wq, tile, 'bias', (bq,))
        ctx_all = attention(qkv, NB, seq_len, heads_a, head_dim)
        attn_sum = scatter_a(times_t(ctx_all, wo, tile, NA))
        x_one = (x_wide + attn_sum + bo).astype(BF16)
        x_one_wide = x_one.astype(F32)
        h_two, normed_two, inv_two = norm_forward(x_one_wide, g2, s2)
        h_two_all = gather_a(h_two)
        pre, act = times(h_two_all, wu, tile, 'gelu', (bu,))

        dy_wide = dy_row.astype(F32)
        part_down, act_down = lax.optimization_barrier((weight_grad(dy_all, act, NB, cols_e), act))
        g_down = reduce_eb(part_down)
        d_pre, gv_up = times(dy_all, wd, tile, 'gelu_grad', (pre,))
        part_up, d_pre = lax.optimization_barrier((weight_grad(h_two_all, d_pre, NB, cols_e), d_pre))
        g_up = reduce_eb(part_up)
        d_h_two = scatter_a(times_t(d_pre, wu, tile, NA)).astype(BF16).astype(F32)
        d_norm_two, gv_g2, gv_s2 = norm_backward(d_h_two, normed_two, inv_two, g2)
        d_x_one = (dy_wide + d_norm_two).astype(BF16)
        d_x_one_wide = d_x_one.astype(F32)
        d_x_all = gather_a(d_x_one)
        d_x_all, act_down = lax.optimization_barrier((d_x_all, act_down))
        down_sum = scatter_a(times_t(act_down, wd, tile, NA))
        y_row = (x_one_wide + down_sum + bd).astype(BF16)
        y_loc = rows_out(y_row)
        d_ctx = times(d_x_all, wo, tile, 'plain')
        d_qkv = attention_grad(qkv, d_ctx, NB, seq_len, heads_a, head_dim)
        gv_qkv = jnp.sum(d_qkv.astype(F32), axis=0)
        part_h, d_qkv = lax.optimization_barrier((times_t(d_qkv, wq, tile, NA), d_qkv))
        d_h_one = scatter_a(part_h).astype(BF16).astype(F32)
        g_qo = reduce_eb_steps(attn_weight_grad(h_one_all, d_qkv, d_x_all, ctx_all, NB, cols_e))
        d_norm_one, gv_g1, gv_s1 = norm_backward(d_h_one, normed_one, inv_one, g1)
        grad_x = rows_out((d_x_one_wide + d_norm_one).astype(BF16))

        def sum_all(rows, per_b):
            spread = [lax.dynamic_update_slice(jnp.zeros((NB, NA, p.size // NB), F32), p.reshape(NB, 1, -1), (0, a_idx, 0)) for p in per_b]
            v = jnp.concatenate([r.reshape(-1) for r in rows] + [t.reshape(-1) for t in spread]).reshape(-1, 128)
            v = v + swap_a(v, 1)
            v = v + swap_a(v, 2)
            v = v + swap_b(v)
            for r in (1, 2):
                v = v + lax.ppermute(v, 'e', [(i, i ^ r) for i in range(NE)])
            v = v.reshape(-1)
            split = len(rows) * NE * cols_e
            mine = [pick(jnp.transpose(v[:split].reshape(len(rows), NE, cols_e), (1, 0, 2)), e_idx)]
            for t in spread:
                mine.append(pick(v[split:split + t.size].reshape(t.shape), b_idx))
                split += t.size
            return mine

        rows = [jnp.sum(dy_wide, axis=0), gv_g2, gv_s2, jnp.sum(d_x_one_wide, axis=0), gv_g1, gv_s1]
        vec, grad_b_up, gq = sum_all(rows, [gv_up, gv_qkv])
        grad_b_up = grad_b_up.reshape(NA * nu)
        gq = gq.reshape(NA, 3, slot)[:, :, :nq].reshape(NA, 3, heads_a, head_dim)
        grad_b_qkv = jnp.transpose(gq, (1, 0, 2, 3)).reshape(3, NA * heads_a, head_dim)

        grad_w_qkv = jnp.stack([g_qo[:, g * slot:g * slot + nq] for g in range(3)])
        grad_w_out = cols_to_rows_a(jnp.concatenate([g_qo[:, g * slot + nq:(g + 1) * slot] for g in range(3)], axis=1))
        grad_w_down = cols_to_rows_a(g_down)
        return (y_loc, grad_x, vec[4], vec[5], grad_w_qkv, grad_b_qkv, grad_w_out, vec[3],
                vec[1], vec[2], g_up, grad_b_up, grad_w_down, vec[0])

    return jax.shard_map(local_step, mesh=mesh, in_specs=all_specs, out_specs=all_specs, check_vma=False)
```

```python
import jax
import jax.numpy as jnp
from jax import lax
from jax.experimental import pallas as pl
from jax.experimental.pallas import tpu as pltpu
from jax.sharding import PartitionSpec as P

LN_EPS = 1e-5
F32 = jnp.float32
BF16 = jnp.bfloat16


def norm_forward(x_wide, gain, shift):
    hidden = x_wide.shape[-1]
    row_mean = jnp.sum(x_wide, axis=-1, keepdims=True) / hidden
    centered = x_wide - row_mean
    variance = jnp.sum(centered * centered, axis=-1, keepdims=True) / hidden
    inv_std = lax.rsqrt(variance + LN_EPS)
    normed = centered * inv_std
    return (normed * gain + shift).astype(BF16), normed, inv_std


def norm_backward(d_out, normed, inv_std, gain):
    hidden = d_out.shape[-1]
    d_normed = d_out * gain
    s0 = jnp.sum(d_normed, axis=-1, keepdims=True) / hidden
    s1 = jnp.sum(d_normed * normed, axis=-1, keepdims=True) / hidden
    d_in = inv_std * (d_normed - s0 - normed * s1)
    return d_in, jnp.sum(d_out * normed, axis=0), jnp.sum(d_out, axis=0)


def lane_ids(shape):
    return lax.broadcasted_iota(jnp.int32, shape, 1)


def head_probs(q_head, k, causal, scale):
    scores = lax.dot_general(q_head, k, (((1,), (1,)), ((), ())), preferred_element_type=F32) * scale
    scores = jnp.where(causal, scores, -1e30)
    probs = jnp.exp(scores - jnp.max(scores, axis=1, keepdims=True))
    return probs * (1.0 / jnp.sum(probs, axis=1, keepdims=True))


def attention_kernel(n_heads, head_dim, qkv_ref, ctx_ref):
    seq_len, slot = ctx_ref.shape
    q, k, v = [qkv_ref[:, g * slot:(g + 1) * slot] for g in range(3)]
    causal = lax.broadcasted_iota(jnp.int32, (seq_len, seq_len), 0) >= lane_ids((seq_len, seq_len))
    lanes = lane_ids((seq_len, slot))
    context = jnp.zeros((seq_len, slot), F32)
    for h in range(n_heads):
        mine = (lanes >= h * head_dim) & (lanes < (h + 1) * head_dim)
        probs = head_probs(jnp.where(mine, q, jnp.zeros_like(q)), k, causal, head_dim ** -0.5).astype(BF16)
        context = jnp.where(mine, jnp.dot(probs, v, preferred_element_type=F32), context)
    ctx_ref[...] = context.astype(BF16)


def attention_grad_kernel(n_heads, head_dim, qkv_ref, dctx_ref, dqkv_ref):
    seq_len, slot = dctx_ref.shape
    q, k, v = [qkv_ref[:, g * slot:(g + 1) * slot] for g in range(3)]
    d_ctx = dctx_ref[...]
    causal = lax.broadcasted_iota(jnp.int32, (seq_len, seq_len), 0) >= lane_ids((seq_len, seq_len))
    lanes = lane_ids((seq_len, slot))
    scale = head_dim ** -0.5
    d_q, d_k, d_v = [jnp.zeros((seq_len, slot), F32) for _ in range(3)]
    for h in range(n_heads):
        mine = (lanes >= h * head_dim) & (lanes < (h + 1) * head_dim)
        q_head = jnp.where(mine, q, jnp.zeros_like(q))
        d_head = jnp.where(mine, d_ctx, jnp.zeros_like(d_ctx))
        probs = head_probs(q_head, k, causal, scale)
        d_v += lax.dot_general(probs.astype(BF16), d_head, (((0,), (0,)), ((), ())), preferred_element_type=F32)
        d_probs = lax.dot_general(d_head, v, (((1,), (1,)), ((), ())), preferred_element_type=F32)
        d_probs = d_probs.astype(BF16).astype(F32)
        d_scores = probs * (d_probs - jnp.sum(d_probs * probs, axis=1, keepdims=True)) * scale
        d_scores = d_scores.astype(BF16)
        d_q = jnp.where(mine, jnp.dot(d_scores, k, preferred_element_type=F32), d_q)
        d_k += lax.dot_general(d_scores, q_head, (((0,), (0,)), ((), ())), preferred_element_type=F32)
    for g, d in enumerate((d_q, d_k, d_v)):
        dqkv_ref[:, g * slot:(g + 1) * slot] = d.astype(BF16)


def attention(qkv, n_b, seq_len, n_heads, head_dim):
    t, width = qkv.shape[0], qkv.shape[1] // n_b
    slot = width // 3
    n = n_b * t // seq_len
    return pl.pallas_call(
        lambda *refs: attention_kernel(n_heads, head_dim, *refs),
        grid=(t // seq_len, n_b),
        out_shape=jax.ShapeDtypeStruct((t, n_b * slot), BF16),
        in_specs=[pl.BlockSpec((seq_len, width), lambda i, j: (i, j))],
        out_specs=pl.BlockSpec((seq_len, slot), lambda i, j: (i, j)),
        cost_estimate=pl.CostEstimate(flops=4 * n * n_heads * seq_len * seq_len * slot, bytes_accessed=n * seq_len * (width + slot) * 2, transcendentals=n * n_heads * seq_len * seq_len),
        name="attention",
    )(qkv)


def attention_grad(qkv, d_ctx, n_b, seq_len, n_heads, head_dim):
    t, width = qkv.shape[0], qkv.shape[1] // n_b
    slot = width // 3
    n = n_b * t // seq_len
    return pl.pallas_call(
        lambda *refs: attention_grad_kernel(n_heads, head_dim, *refs),
        grid=(t // seq_len, n_b),
        out_shape=jax.ShapeDtypeStruct(qkv.shape, BF16),
        in_specs=[pl.BlockSpec((seq_len, width), lambda i, j: (i, j)),
                  pl.BlockSpec((seq_len, slot), lambda i, j: (i, j))],
        out_specs=pl.BlockSpec((seq_len, width), lambda i, j: (i, j)),
        cost_estimate=pl.CostEstimate(flops=10 * n * n_heads * seq_len * seq_len * slot, bytes_accessed=n * seq_len * (2 * width + slot) * 2, transcendentals=n * n_heads * seq_len * seq_len),
        name="attention_grad",
    )(qkv, d_ctx)


def cat(refs):
    return jnp.concatenate([r[...] for r in refs], axis=0)


def tn(left, right):
    return lax.dot_general(left, right, (((0,), (0,)), ((), ())), preferred_element_type=F32)


def weight_grad(lefts, right, b, block):
    m, k = lefts[0].shape
    t = m * len(lefts)
    n = right.shape[1] // b

    def kernel(*refs):
        refs[-1][0] = tn(cat(refs[:-2]), refs[-2][...]).astype(BF16)

    return pl.pallas_call(
        kernel,
        grid=(b, k // block),
        out_shape=jax.ShapeDtypeStruct((b, k, n), BF16),
        in_specs=[pl.BlockSpec((m, block), lambda i, j: (0, j))] * len(lefts) + [pl.BlockSpec((t, n), lambda i, j: (0, i))],
        out_specs=pl.BlockSpec((1, block, n), lambda i, j: (i, j, 0)),
        cost_estimate=pl.CostEstimate(flops=2 * b * t * k * n, bytes_accessed=2 * (b * t * k + b * t * n + b * k * n), transcendentals=0),
        name="weight_grad",
    )(*lefts, right)


def attn_weight_grad(hs, d_qkv, d_xs, ctx, b, block):
    m, k = hs[0].shape
    parts = len(hs)
    t = m * parts
    n = d_qkv.shape[1] // b
    slot = n // 3
    used = slot * 3 // 4

    def kernel(*refs):
        h, d_x = cat(refs[:parts]), cat(refs[parts:2 * parts])
        dqkv_ref, ctx_ref, out_ref = refs[2 * parts:]
        d_out = tn(d_x, ctx_ref[...])
        lanes = lane_ids(d_out.shape)
        for g in range(3):
            moved = pltpu.roll(d_out, (used - g * (slot - used)) % slot, 1)
            d = tn(h, dqkv_ref[:, g * slot:(g + 1) * slot])
            out_ref[0, :, g * slot:(g + 1) * slot] = jnp.where(lanes >= used, moved, d).astype(BF16)

    return pl.pallas_call(
        kernel,
        grid=(b, k // block),
        out_shape=jax.ShapeDtypeStruct((b, k, n), BF16),
        in_specs=[pl.BlockSpec((m, block), lambda i, j: (0, j))] * (2 * parts)
        + [pl.BlockSpec((t, n), lambda i, j: (0, i)), pl.BlockSpec((t, slot), lambda i, j: (0, i))],
        out_specs=pl.BlockSpec((1, block, n), lambda i, j: (i, j, 0)),
        cost_estimate=pl.CostEstimate(flops=2 * b * t * k * (n + slot), bytes_accessed=2 * (2 * b * t * k + b * t * n + b * k * n), transcendentals=0),
        name="attn_weight_grad",
    )(*hs, *d_xs, d_qkv, ctx)


GELU_C = 0.7978845608028654


def times(lefts, w, tile, epilogue, extras=(), cols=None):
    m, k = lefts[0].shape
    parts = len(lefts)
    t = m * parts
    b = w.shape[0]
    first, n = cols or (0, w.shape[2])
    first, steps = first // tile, n // tile
    wide = lambda i, j: (0, i * steps + j)
    outs = {'plain': [(t, BF16)], 'bias': [(t, BF16)], 'gelu': [(t, F32), (t, BF16)], 'gelu_grad': [(t, BF16), (1, F32)]}[epilogue]

    def kernel(*refs):
        w_ref = refs[parts]
        extra = refs[parts + 1:parts + 1 + len(extras)]
        out = refs[parts + 1 + len(extras):-1]
        rows = refs[-1]

        @pl.when((pl.program_id(0) == 0) & (pl.program_id(1) == 0))
        def _():
            for r in range(parts):
                rows[r * m:(r + 1) * m, :] = refs[r][...]

        y = jnp.dot(rows[...], w_ref[0], preferred_element_type=F32)
        if epilogue == 'plain':
            out[0][...] = y.astype(BF16)
        elif epilogue == 'bias':
            out[0][...] = (y + extra[0][...]).astype(BF16)
        elif epilogue == 'gelu':
            y = y + extra[0][...]
            out[0][...] = y
            out[1][...] = (y * (0.5 * (1.0 + jnp.tanh(GELU_C * (y + 0.044715 * (y * y * y)))))).astype(BF16)
        else:
            d = y.astype(BF16).astype(F32)
            x = extra[0][...]
            th = jnp.tanh(GELU_C * (x + 0.044715 * (x * x * x)))
            slope = 0.5 * (1.0 + th) + 0.5 * x * (1.0 - th * th) * (GELU_C * (1.0 + 3 * 0.044715 * (x * x)))
            d = d * slope
            out[0][...] = d.astype(BF16)
            out[1][...] = jnp.sum(d, axis=0, keepdims=True)

    res = pl.pallas_call(
        kernel,
        grid=(b, steps),
        out_shape=[jax.ShapeDtypeStruct((r, b * n), d) for r, d in outs],
        in_specs=[pl.BlockSpec((m, k), lambda i, j: (0, 0))] * parts + [pl.BlockSpec((1, k, tile), lambda i, j: (i, 0, first + j))]
        + [pl.BlockSpec((x.shape[0], tile), wide) for x in extras],
        out_specs=[pl.BlockSpec((r, tile), wide) for r, d in outs],
        scratch_shapes=[pltpu.VMEM((t, k), BF16)],
        cost_estimate=pl.CostEstimate(flops=2 * b * t * k * n, bytes_accessed=2 * (t * k + b * k * n + 2 * b * t * n), transcendentals=0),
    )(*lefts, w, *extras)
    return res[0] if len(outs) == 1 else res


def times_t(left, w, tile, parts, cols=None):
    t = left.shape[0]
    b, k, _ = w.shape
    first, n = cols or (0, w.shape[2])
    first = first // n
    m = t // parts

    def kernel(left_ref, w_ref, *out):
        y = sum(lax.dot_general(left_ref[:, i * n:(i + 1) * n], w_ref[i], (((1,), (1,)), ((), ())), preferred_element_type=F32) for i in range(b))
        for r in range(parts):
            out[r][...] = y[r * m:(r + 1) * m].astype(BF16)

    return pl.pallas_call(
        kernel,
        grid=(k // tile,),
        out_shape=[jax.ShapeDtypeStruct((m, k), BF16)] * parts,
        in_specs=[pl.BlockSpec((t, b * n), lambda j: (0, 0)), pl.BlockSpec((b, tile, n), lambda j: (0, j, first))],
        out_specs=[pl.BlockSpec((m, tile), lambda j: (0, j))] * parts,
        cost_estimate=pl.CostEstimate(flops=2 * b * t * k * n, bytes_accessed=2 * (t * k + b * k * n + b * t * n), transcendentals=0),
        name="times_t",
    )(left, w)


def solution(mesh):
    NE, NB, NA = mesh.shape['e'], mesh.shape['b'], mesh.shape['a']
    spec_act = P(('a', 'b'), None, 'e')
    spec_col_e = P('e')
    spec_col_b = P('b')
    spec_qkv = P(None, 'e', ('b', 'a'))
    spec_qkv_bias = P(None, 'b', None)
    spec_rows_b = P('b', ('e', 'a'))
    spec_rows_e = P('e', ('b', 'a'))
    all_specs = (spec_act, spec_act, spec_col_e, spec_col_e, spec_qkv, spec_qkv_bias, spec_rows_b,
                 spec_col_e, spec_col_e, spec_col_e, spec_rows_e, spec_col_b, spec_rows_b, spec_col_e)

    def from_e(t, k):
        return lax.ppermute(t, 'e', [((i + k) % NE, i) for i in range(NE)])

    def to_e(t, k):
        return lax.ppermute(t, 'e', [(i, (i + k) % NE) for i in range(NE)])

    def swap_b(t):
        return lax.ppermute(t, 'b', [(0, 1), (1, 0)])

    def swap_x(t):
        return swap_a(t, 2)

    def swap_a(t, r):
        return lax.ppermute(t, 'a', [(i, i ^ r) for i in range(NA)])

    def pick(t, i):
        return lax.dynamic_index_in_dim(t, i, 0, keepdims=False)

    def local_step(x_loc, dy_loc, ln1_gain, ln1_shift, w_qkv, b_qkv, w_out, b_out, ln2_gain, ln2_shift, w_up, b_up, w_down, b_down):
        e_idx, b_idx, a_idx = lax.axis_index('e'), lax.axis_index('b'), lax.axis_index('a')
        _, seq_len, cols_e = x_loc.shape
        heads_b, head_dim = b_qkv.shape[1], b_qkv.shape[2]
        heads_a = heads_b // NA

        def rows_in(t):
            got = [pick(t, e_idx)]
            got += [from_e(pick(t, (e_idx - k) % NE), k) for k in range(1, NE)]
            got = jnp.stack(got)
            return jnp.concatenate([pick(got, (j - e_idx) % NE) for j in range(NE)], axis=-1)

        def rows_out(t):
            blocks = jnp.stack([t[:, j * cols_e:(j + 1) * cols_e] for j in range(NE)])
            got = [pick(blocks, e_idx)] + [to_e(pick(blocks, (e_idx + k) % NE), k) for k in range(1, NE)]
            got = jnp.stack(got)
            return jnp.stack([pick(got, (e_idx - j) % NE) for j in range(NE)])

        def gather_eb(blk):
            full = lax.all_gather(blk, ('b', 'e'), axis=0, tiled=True)
            return full.reshape(NB, NE * blk.shape[0], blk.shape[1])

        def reduce_eb(part):
            return lax.psum_scatter(part.reshape(NB * part.shape[1], part.shape[2]), ('b', 'e'), scatter_dimension=0, tiled=True)

        def gather_ex_steps(blk):
            full = jnp.zeros((2, NE) + blk.shape, blk.dtype)
            for k in range(NE):
                for p, t in ((0, blk), (1, swap_x(blk))):
                    full = lax.dynamic_update_slice(full, t[None, None], (p, (e_idx + k) % NE, 0, 0))
                if k < NE - 1:
                    blk = from_e(blk, 1)
            return full.reshape(2, NE * blk.shape[0], blk.shape[1])

        def reduce_ex_steps(part):
            part = part.reshape(2, NE, cols_e, part.shape[2])
            order = (1, 3, 2, 0)
            total = {k: pick(part[0], (e_idx + k) % NE).astype(F32) + swap_x(pick(part[1], (e_idx + k) % NE)).astype(F32) for k in order}
            out = total[0]
            for k in (1, 3, 2):
                out = out + to_e(total[k].astype(BF16), k).astype(F32)
            return out.astype(BF16)

        def gather_t(t, far):
            t2 = far(t)
            return [t, swap_a(t, 1), t2, swap_a(t2, 1)]

        def scatter_t(parts, far):
            p0, p1, p2, p3 = parts
            q2 = (p2.astype(F32) + swap_a(p3, 1).astype(F32)).astype(BF16)
            got = far(q2)
            return p0.astype(F32) + swap_a(p1, 1).astype(F32) + got.astype(F32)

        def rows_to_cols_a(w):
            blocks = w.reshape(NA, w.shape[0] // NA, w.shape[1])
            blocks = jnp.transpose(blocks, (0, 2, 1))
            rel = [pick(blocks, a_idx)] + [swap_a(pick(blocks, a_idx ^ r), r) for r in range(1, NA)]
            rel = jnp.stack(rel)
            return jnp.concatenate([pick(rel, j ^ a_idx) for j in range(NA)], axis=0)

        def cols_to_rows_a(w):
            blocks = w.reshape(NA, w.shape[0] // NA, w.shape[1])
            rel = [pick(blocks, a_idx)] + [swap_a(pick(blocks, a_idx ^ r), r) for r in range(1, NA)]
            rel = jnp.stack(rel)
            rel = jnp.stack([pick(rel, j ^ a_idx) for j in range(NA)])
            return jnp.transpose(rel, (0, 2, 1)).reshape(NA * w.shape[1], w.shape[0] // NA)

        nq = w_qkv.shape[2]
        nfill = nq // 3
        out_blk = rows_to_cols_a(w_out)
        qo_blk = jnp.concatenate([t for g in range(3) for t in (w_qkv[g], out_blk[:, g * nfill:(g + 1) * nfill])], axis=1)
        slot = nq + nfill
        wq = gather_ex_steps(qo_blk)
        wo = jnp.concatenate([wq[:, :, g * slot + nq:(g + 1) * slot] for g in range(3)] + [jnp.zeros((NB, wq.shape[1], nfill), BF16)], axis=2)
        x_row = rows_in(x_loc)
        mlp_blk = jnp.concatenate([w_up, rows_to_cols_a(w_down)], axis=1)
        x_row, mlp_blk = lax.optimization_barrier((x_row, mlp_blk))
        wm = gather_eb(mlp_blk)
        nu = w_up.shape[1]
        up_cols, down_cols = (0, nu), (nu, nu)
        vecs = jnp.stack([ln1_gain, ln1_shift, ln2_gain, ln2_shift, b_out, b_down])
        vecs = jnp.stack([vecs] + [from_e(vecs, k) for k in range(1, NE)])
        vecs = jnp.concatenate([pick(vecs, (j - e_idx) % NE) for j in range(NE)], axis=1)
        g1, s1, g2, s2, bo, bd = [vecs[i:i + 1] for i in range(6)]

        def both_b(v):
            other = swap_b(v)
            return jnp.stack([jnp.where(b_idx == 0, v, other), jnp.where(b_idx == 0, other, v)])

        bq = jnp.transpose(b_qkv.reshape(3, NA, nq), (1, 0, 2))
        bq = jnp.pad(jnp.stack([pick(bq, a_idx), pick(bq, a_idx ^ 2)]), ((0, 0), (0, 0), (0, nfill))).reshape(1, 2 * 3 * slot)
        bu = both_b(lax.dynamic_index_in_dim(b_up.reshape(NA, b_up.shape[0] // NA), a_idx, 0, keepdims=True)).reshape(1, NB * nu)

        tile = slot

        x_wide = x_row.astype(F32)
        h_one, normed_one, inv_one = norm_forward(x_wide, g1, s1)
        h_one_all = gather_t(h_one, swap_b)
        qkv = times(h_one_all, wq, tile, 'bias', (bq,))
        qkv, dy_loc = lax.optimization_barrier((qkv, dy_loc))
        dy_row = rows_in(dy_loc)
        dy_all = gather_t(dy_row, swap_x)
        ctx_all = attention(qkv, NB, seq_len, heads_a, head_dim)
        attn_sum = scatter_t(times_t(ctx_all, wo, tile, NA), swap_b)
        x_one = (x_wide + attn_sum + bo).astype(BF16)
        x_one_wide = x_one.astype(F32)
        h_two, normed_two, inv_two = norm_forward(x_one_wide, g2, s2)
        h_two_all = gather_t(h_two, swap_x)
        pre, act = times(h_two_all, wm, tile, 'gelu', (bu,), up_cols)

        dy_wide = dy_row.astype(F32)
        part_down, act_down = lax.optimization_barrier((weight_grad(dy_all, act, NB, cols_e), act))
        g_down = reduce_eb(part_down)
        d_pre, gv_up = times(dy_all, wm, tile, 'gelu_grad', (pre,), down_cols)
        part_h, d_pre = lax.optimization_barrier((times_t(d_pre, wm, tile, NA, up_cols), d_pre))
        d_h_two = scatter_t(part_h, swap_x).astype(BF16).astype(F32)
        part_up = weight_grad(h_two_all, d_pre, NB, cols_e)
        g_up = reduce_eb(part_up)
        d_norm_two, gv_g2, gv_s2 = norm_backward(d_h_two, normed_two, inv_two, g2)
        d_x_one = (dy_wide + d_norm_two).astype(BF16)
        d_x_one_wide = d_x_one.astype(F32)
        act_down, d_x_one = lax.optimization_barrier((act_down, d_x_one))
        d_x_all = gather_t(d_x_one, swap_b)
        part_y = times_t(act_down, wm, tile, NA, down_cols)
        down_sum = scatter_t(part_y, swap_x)
        y_row = (x_one_wide + down_sum + bd).astype(BF16)
        y_loc = rows_out(y_row)
        d_ctx = times(d_x_all, wo, tile, 'plain')
        d_qkv = attention_grad(qkv, d_ctx, NB, seq_len, heads_a, head_dim)
        gv_qkv = jnp.sum(d_qkv.astype(F32), axis=0)
        part_h, d_qkv = lax.optimization_barrier((times_t(d_qkv, wq, tile, NA), d_qkv))
        d_h_one = scatter_t(part_h, swap_b).astype(BF16).astype(F32)
        part_qo = attn_weight_grad(h_one_all, d_qkv, d_x_all, ctx_all, NB, cols_e)
        g_qo = reduce_ex_steps(part_qo)
        d_norm_one, gv_g1, gv_s1 = norm_backward(d_h_one, normed_one, inv_one, g1)
        grad_x = rows_out((d_x_one_wide + d_norm_one).astype(BF16))

        def sum_all(rows, up, qkv_cols):
            up = lax.dynamic_update_slice(jnp.zeros((NB, NA, up.size // NB), F32), up.reshape(NB, 1, -1), (0, a_idx, 0))
            qkv_cols = qkv_cols.reshape(2, 1, 1, -1)
            spread = jnp.zeros((NB, NA, qkv_cols.shape[3]), F32)
            spread = lax.dynamic_update_slice(spread, qkv_cols[0], (b_idx, a_idx, 0))
            spread = [up, lax.dynamic_update_slice(spread, qkv_cols[1], (b_idx, a_idx ^ 2, 0))]
            v = jnp.concatenate([r.reshape(-1) for r in rows] + [t.reshape(-1) for t in spread]).reshape(-1, 128)
            v = v + swap_a(v, 1)
            v = v + swap_a(v, 2)
            v = v + swap_b(v)
            for r in (1, 2):
                v = v + lax.ppermute(v, 'e', [(i, i ^ r) for i in range(NE)])
            v = v.reshape(-1)
            split = len(rows) * NE * cols_e
            mine = [pick(jnp.transpose(v[:split].reshape(len(rows), NE, cols_e), (1, 0, 2)), e_idx)]
            for t in spread:
                mine.append(pick(v[split:split + t.size].reshape(t.shape), b_idx))
                split += t.size
            return mine

        rows = [jnp.sum(dy_wide, axis=0), gv_g2, gv_s2, jnp.sum(d_x_one_wide, axis=0), gv_g1, gv_s1]
        vec, grad_b_up, gq = sum_all(rows, gv_up, gv_qkv)
        grad_b_up = grad_b_up.reshape(NA * nu)
        gq = gq.reshape(NA, 3, slot)[:, :, :nq].reshape(NA, 3, heads_a, head_dim)
        grad_b_qkv = jnp.transpose(gq, (1, 0, 2, 3)).reshape(3, NA * heads_a, head_dim)

        grad_w_qkv = jnp.stack([g_qo[:, g * slot:g * slot + nq] for g in range(3)])
        grad_w_out = cols_to_rows_a(jnp.concatenate([g_qo[:, g * slot + nq:(g + 1) * slot] for g in range(3)], axis=1))
        grad_w_down = cols_to_rows_a(g_down)
        return (y_loc, grad_x, vec[4], vec[5], grad_w_qkv, grad_b_qkv, grad_w_out, vec[3],
                vec[1], vec[2], g_up, grad_b_up, grad_w_down, vec[0])

    return jax.shard_map(local_step, mesh=mesh, in_specs=all_specs, out_specs=all_specs, check_vma=False)
```
